256 devices in a mesh: groups: 4 (over y, x), gx: 64 (over z, core).
Axes of the slice: x: 2, y: 2, z: 32, core: 2. Of those that a mesh axis runs over, the one named last changes fastest.
The devices are a block of a 4x8x32 slice.
Arguments:
- tokens: bfloat16 [1536, 4608], P('groups', 'gx'), parts along dimension 0, may hold values from -6 to 6
- gate_weight: bfloat16 [64, 576, 2304], P('gx'), may hold values from -0.09375 to 0.09375
- up_weight: bfloat16 [64, 576, 2304], P('gx'), may hold values from -0.09375 to 0.09375
- down_weight: bfloat16 [64, 2304, 576], P('gx'), may hold values from -0.046875 to 0.046875
Outputs:
- mixed: bfloat16 [1536, 4608], P('groups', 'gx'), parts along dimension 0
The draws below stay inside these ranges and needn't reach their ends.
There are 4 independent parts, one for each index of `groups`. The reference program is written for one: setup_inputs(seed, part) draws one part's arguments, and reference() takes and returns one part's arrays. A program takes and returns all parts, laid end to end along the dimension named above; an argument that names none is the same for every part. Nothing has to cross between parts.
All inputs are finite; a program needn't handle non-finite values.
Results may differ from the reference program's by a relative error of at most 0.015.
Values may be sent and summed in bfloat16 or wider, within the bound.
A program may use at most 128 MiB of HBM per device.

```python
import jax
import jax.numpy as jnp

D = 4608
FF = 18432
TOK = 384
XS = 8
YS = 8


def level_of(own_key, shape, cuts, smallest, top_value):
    gain = 1.0
    for position, parts in cuts:
        draws = jax.random.uniform(jax.random.fold_in(jax.random.fold_in(own_key, 6), position), (parts,), jnp.float32, smallest / len(cuts), top_value / len(cuts))
        gain = gain * jnp.repeat(jnp.exp(draws), shape[position] // parts).reshape((-1,) + (1,) * (len(shape) - 1 - position))
    return gain


def scatter_about(rng, shape, spread, reach, cuts=(), kind=jnp.bfloat16):
    result = spread * jax.random.normal(rng, shape, jnp.float32)
    if cuts:
        result = result * level_of(rng, shape, cuts, -0.22, 0.18)
    return jnp.clip(result, -reach, reach).astype(kind)


def setup_inputs(seed: int = 0, part: int = 0) -> dict:
    splits = jax.random.split(jax.random.key(seed), 5)
    part_splits = jax.random.split(jax.random.fold_in(splits[4], part), 5)
    tokens = scatter_about(part_splits[0], (TOK, D), 1.0, 6.0, ((1, 64),))
    gate_weight = scatter_about(splits[1], (XS * YS, D // XS, FF // YS), D ** -0.5, 0.09375, ((0, 64),))
    up_weight = scatter_about(splits[2], (XS * YS, D // XS, FF // YS), D ** -0.5, 0.09375, ((0, 64),))
    down_weight = scatter_about(splits[3], (XS * YS, FF // XS, D // YS), FF ** -0.5, 0.046875, ((0, 64),))
    return {"tokens": tokens, "gate_weight": gate_weight, "up_weight": up_weight, "down_weight": down_weight}


def assemble(tile_stack, row_count, column_count):
    blocks = tile_stack.reshape(YS, XS, YS, -1, tile_stack.shape[2])
    return blocks.transpose(2, 1, 3, 0, 4).reshape(row_count, column_count)


def reference(tokens, gate_weight, up_weight, down_weight):
    gate_full = assemble(gate_weight, D, FF)
    up_full = assemble(up_weight, D, FF)
    down_full = assemble(down_weight, FF, D)
    gate = jnp.dot(tokens, gate_full, preferred_element_type=jnp.float32)
    up_proj = jnp.dot(tokens, up_full, preferred_element_type=jnp.float32)
    hidden = (jax.nn.gelu(gate, approximate=True) * up_proj).astype(jnp.bfloat16)
    mixed = jnp.dot(hidden, down_full, preferred_element_type=jnp.float32)
    return mixed.astype(jnp.bfloat16)
```

```python
import functools

import jax
import jax.numpy as jnp
from jax import lax
from jax.experimental import pallas as pl
from jax.experimental.pallas import tpu as pltpu
from jax.sharding import PartitionSpec as P

XS = 8
CORES = 2
Q = XS // CORES
TSPLIT = 3
SSPLIT = 3
MESH = pl.DeviceIdType.MESH


def gelu(v):
    return 0.5 * v * (1.0 + jnp.tanh(0.7978845608 * (v + 0.044715 * v * v * v)))


def kernel(
    G,
    tok_ref,
    gate_hbm,
    up_hbm,
    down_hbm,
    out_ref,
    w_v,
    d_v,
    wt,
    tok,
    x32,
    xb,
    sib_send,
    sib_recv,
    own,
    ch_send,
    ch_recv,
    hbuf,
    acc,
    o_sib_send,
    o_sib_recv,
    o_send,
    o_recv,
    load_sem,
    tok_ss,
    tok_rs,
    sib_ss,
    sib_rs,
    ch_ss,
    ch_rs,
    h_ss,
    h_rs,
    os_ss,
    os_rs,
    o_ss,
    o_rs,
):
    S, T = SSPLIT, TSPLIT
    f = tok_ref.shape[1]
    tokens = tok_ref.shape[0]
    tl = tokens // T
    R = hbuf.shape[2]
    HB = R * S

    me = lax.axis_index("gx")
    a = me // XS
    b = lax.rem(me, XS)
    p = b // CORES
    core = lax.rem(b, CORES)

    step = 1 - 2 * core
    long_n = G // 2
    short_n = G - 1 - long_n
    group_at = lambda k: lax.rem(a + k * step + G, G)
    long_to = group_at(1) * XS + b
    short_to = group_at(-1) * XS + b
    sibling = a * XS + p * CORES + (1 - core)
    chip = lambda q: a * XS + q * CORES + core
    to = lambda index: {"gx": index}

    loads = [
        pltpu.make_async_copy(gate_hbm.at[0], w_v.at[0], load_sem.at[0]),
        pltpu.make_async_copy(up_hbm.at[0], w_v.at[1], load_sem.at[1]),
        pltpu.make_async_copy(down_hbm.at[0], d_v, load_sem.at[2]),
    ]
    for c in loads:
        c.start()

    own_t = tok_ref[...].astype(jnp.float32).T.astype(jnp.bfloat16)
    for t in range(T):
        tok[t, a] = own_t[:, t * tl : (t + 1) * tl]

    barrier = pltpu.get_barrier_semaphore()
    peers = [long_to, short_to, sibling] + [chip(lax.rem(p + j, Q)) for j in range(1, Q)]
    for peer in peers:
        pl.semaphore_signal(barrier, inc=1, device_id=to(peer), device_id_type=MESH)
    pl.semaphore_wait(barrier, len(peers))

    def remote(src, dst, ss, rs, peer):
        return pltpu.make_async_remote_copy(
            src_ref=src, dst_ref=dst, send_sem=ss, recv_sem=rs, device_id=to(peer), device_id_type=MESH
        )

    def ring(buf, ss, rs, i, k, far):
        if far:
            c, peer, e = group_at(-(k - 1)), long_to, k - 1
        else:
            c, peer, e = group_at(k - 1), short_to, long_n + k - 1
        return remote(buf.at[i, c], buf.at[i, c], ss.at[i, e], rs.at[i, e], peer)

    def ring_step(buf, ss, rs, i, k):
        ring(buf, ss, rs, i, k, True).wait_recv()
        if k < long_n:
            ring(buf, ss, rs, i, k + 1, True).start()
        if k <= short_n:
            ring(buf, ss, rs, i, k, False).wait_recv()
            if k < short_n:
                ring(buf, ss, rs, i, k + 1, False).start()

    def ring_start(buf, ss, rs, i):
        ring(buf, ss, rs, i, 1, True).start()
        if short_n:
            ring(buf, ss, rs, i, 1, False).start()

    def ring_drain(buf, ss, rs, i):
        for k in range(1, long_n + 1):
            ring(buf, ss, rs, i, k, True).wait_send()
        for k in range(1, short_n + 1):
            ring(buf, ss, rs, i, k, False).wait_send()

    for t in range(T):
        ring_start(tok, tok_ss, tok_rs, t)

    def turn(g):
        loads[g].wait()
        wide = 128

        def body(j, carry):
            j0 = pl.multiple_of(j * wide, wide)
            wt[g, pl.ds(j0, wide), :] = w_v[g, :, pl.ds(j0, wide)].T
            return carry

        lax.fori_loop(0, w_v.shape[2] // wide, body, 0)

    turn(0)
    for t in range(T):
        ring_step(tok, tok_ss, tok_rs, t, 1)
    turn(1)
    for k in range(2, long_n + 1):
        for t in range(T):
            ring_step(tok, tok_ss, tok_rs, t, k)
    loads[2].wait()

    for t in range(T):
        for c in range(G):
            x32[c * f : (c + 1) * f, t * tl : (t + 1) * tl] = tok[t, c].astype(jnp.float32)
    xb[...] = x32[...].astype(jnp.bfloat16)

    def part(q, g, of_core):
        row = pl.multiple_of((q * CORES + of_core) * HB, 32)
        return jnp.dot(wt[g, pl.ds(row, HB), :], xb[...], preferred_element_type=jnp.float32)

    def sib_part(i, carry):
        q, g = i // 2, lax.rem(i, 2)
        r = part(q, g, 1 - core).astype(jnp.bfloat16)
        for s in range(S):
            sib_send[s, q, g] = r[s * R : (s + 1) * R]
        return carry

    lax.fori_loop(0, Q * 2, sib_part, 0)
    sib = [remote(sib_send.at[s], sib_recv.at[s], sib_ss.at[s], sib_rs.at[s], sibling) for s in range(S)]
    for s in range(S):
        sib[s].start()

    def own_part(i, carry):
        q, g = i // 2, lax.rem(i, 2)
        r = part(q, g, core)
        for s in range(S):
            own[s, q, g] = r[s * R : (s + 1) * R]
        return carry

    lax.fori_loop(0, Q * 2, own_part, 0)

    def chain(d, s, q):
        peer = chip(p + 1) if d == 0 else chip(p - 1)
        return remote(ch_send.at[d, s, q], ch_recv.at[d, s, q], ch_ss.at[d, s, q], ch_rs.at[d, s, q], peer)

    def chain_from(d, s, q):
        peer = chip(p - 1) if d == 0 else chip(p + 1)
        return remote(ch_send.at[d, s, q], ch_recv.at[d, s, q], ch_ss.at[d, s, q], ch_rs.at[d, s, q], peer)

    def is_first(d):
        return p == 0 if d == 0 else p == Q - 1

    def sends(d, q):
        return p < q if d == 0 else p > q

    order = []
    for j in range(Q - 1):
        order += [(0, Q - 1 - j), (1, j)]

    def chain_all(s):
        sib[s].wait_recv()
        for d, q in order:

            @pl.when(jnp.logical_and(is_first(d), sends(d, q)))
            def _():
                ch_send[d, s, q] = (own[s, q] + sib_recv[s, q].astype(jnp.float32)).astype(jnp.bfloat16)
                chain(d, s, q).start()

            @pl.when(jnp.logical_and(jnp.logical_not(is_first(d)), sends(d, q)))
            def _():
                v = own[s, q] + sib_recv[s, q].astype(jnp.float32)
                chain_from(d, s, q).wait_recv()
                ch_send[d, s, q] = (v + ch_recv[d, s, q].astype(jnp.float32)).astype(jnp.bfloat16)
                chain(d, s, q).start()

        own[s, p] = own[s, p] + sib_recv[s, p].astype(jnp.float32)
        for d in range(2):

            @pl.when(jnp.logical_not(is_first(d)))
            def _():
                chain_from(d, s, p).wait_recv()
                own[s, p] = own[s, p] + ch_recv[d, s, p].astype(jnp.float32)

        hbuf[s, a] = (gelu(own[s, p, 0]) * own[s, p, 1]).astype(jnp.bfloat16)
        ring_start(hbuf, h_ss, h_rs, s)

    def chain_drain(s):
        for d, q in order:

            @pl.when(sends(d, q))
            def _():
                chain(d, s, q).wait_send()

    acc[...] = jnp.zeros_like(acc)

    def down(s, c):
        row = pl.multiple_of(c * HB + s * R, 16)
        acc[...] += lax.dot_general(
            d_v[pl.ds(row, R), :], hbuf[s, c], (((0,), (0,)), ((), ())), preferred_element_type=jnp.float32
        )

    def h_step(s, k):
        ring_step(hbuf, h_ss, h_rs, s, k)
        down(s, group_at(-k))
        if k <= short_n:
            down(s, group_at(k))

    for s in range(S):
        chain_all(s)
        down(s, a)
        for j in range(1, s + 1):
            h_step(s - j, j)
    for w in range(S, S + long_n):
        for s in reversed(range(S)):
            if 1 <= w - s <= long_n:
                h_step(s, w - s)

    def block(bb):
        return acc[pl.ds(pl.multiple_of(bb * f, 8), f), :]

    for q in range(Q):
        o_sib_send[q] = block(q * CORES + 1 - core).astype(jnp.bfloat16)
    osib = remote(o_sib_send, o_sib_recv, os_ss, os_rs, sibling)
    osib.start()
    osib.wait_recv()
    outs = []
    for j in range(1, Q):
        q = lax.rem(p + j, Q)
        o_send[j - 1] = (block(q * CORES + core) + o_sib_recv[q].astype(jnp.float32)).astype(jnp.bfloat16)
        c = remote(o_send.at[j - 1], o_recv.at[j - 1], o_ss.at[j - 1], o_rs.at[j - 1], chip(q))
        c.start()
        outs.append(c)
    total = block(b) + o_sib_recv[p].astype(jnp.float32)
    for j, c in enumerate(outs):
        c.wait_recv()
        total = total + o_recv[j].astype(jnp.float32)
    out_ref[...] = total.T.astype(jnp.bfloat16)

    for t in range(T):
        ring_drain(tok, tok_ss, tok_rs, t)
    for s in range(S):
        sib[s].wait_send()
        chain_drain(s)
        ring_drain(hbuf, h_ss, h_rs, s)
    osib.wait_send()
    for c in outs:
        c.wait_send()


def shards(G, tokens, gate_weight, up_weight, down_weight):
    rows, f = tokens.shape
    _, depth, width = gate_weight.shape
    _, down_depth, out_width = down_weight.shape
    hb = width // XS
    R = hb // SSPLIT
    bf, f32 = jnp.bfloat16, jnp.float32
    dma = pltpu.SemaphoreType.DMA
    V = pltpu.VMEM
    return pl.pallas_call(
        functools.partial(kernel, G),
        out_shape=jax.ShapeDtypeStruct((rows, f), bf),
        in_specs=[pl.BlockSpec(memory_space=pltpu.VMEM)] + [pl.BlockSpec(memory_space=pl.ANY)] * 3,
        out_specs=pl.BlockSpec(memory_space=pltpu.VMEM),
        scratch_shapes=[
            V((2, depth, width), bf),
            V((down_depth, out_width), bf),
            V((2, width, depth), bf),
            V((TSPLIT, G, f, rows // TSPLIT), bf),
            V((depth, rows), f32),
            V((depth, rows), bf),
            V((SSPLIT, Q, 2, R, rows), bf),
            V((SSPLIT, Q, 2, R, rows), bf),
            V((SSPLIT, Q, 2, R, rows), f32),
            V((2, SSPLIT, Q, 2, R, rows), bf),
            V((2, SSPLIT, Q, 2, R, rows), bf),
            V((SSPLIT, G, R, rows), bf),
            V((out_width, rows), f32),
            V((Q, f, rows), bf),
            V((Q, f, rows), bf),
            V((Q - 1, f, rows), bf),
            V((Q - 1, f, rows), bf),
            dma((3,)),
            dma((TSPLIT, G - 1)),
            dma((TSPLIT, G - 1)),
            dma((SSPLIT,)),
            dma((SSPLIT,)),
            dma((2, SSPLIT, Q)),
            dma((2, SSPLIT, Q)),
            dma((SSPLIT, G - 1)),
            dma((SSPLIT, G - 1)),
            dma(()),
            dma(()),
            dma((Q - 1,)),
            dma((Q - 1,)),
        ],
        compiler_params=pltpu.CompilerParams(
            collective_id=0, has_side_effects=True, vmem_limit_bytes=60 * 1024 * 1024
        ),
    )(tokens, gate_weight, up_weight, down_weight)


def solution(mesh):
    G = mesh.shape["gx"] // XS
    placed = (P("groups", "gx"), P("gx", None, None), P("gx", None, None), P("gx", None, None))
    return jax.shard_map(
        functools.partial(shards, G), mesh=mesh, in_specs=placed, out_specs=P("groups", "gx"), check_vma=False
    )
```

```python
import contextlib
import functools

import jax
import jax.numpy as jnp
from jax import lax
from jax.experimental import pallas as pl
from jax.experimental.pallas import tpu as pltpu
from jax.sharding import PartitionSpec as P

XS = 8
CORES = 2
Q = XS // CORES
TSPLIT = 3
SSPLIT = 3
HOLD = 5
PACE = 1.5
MESH = pl.DeviceIdType.MESH


def scope(name):
    return contextlib.nullcontext()


def gelu(v):
    return 0.5 * v * (1.0 + jnp.tanh(0.7978845608 * (v + 0.044715 * v * v * v)))


def kernel(
    G,
    tok_ref,
    gate_hbm,
    up_hbm,
    down_hbm,
    out_ref,
    w_v,
    dt_v,
    d_v,
    wt,
    tok,
    x32,
    xb,
    sib_send,
    sib_recv,
    own,
    ch_send,
    ch_recv,
    hbuf,
    acc,
    o_sib_send,
    o_sib_recv,
    o_send,
    o_recv,
    load_sem,
    tok_ss,
    tok_rs,
    sib_ss,
    sib_rs,
    ch_ss,
    ch_rs,
    h_ss,
    h_rs,
    os_ss,
    os_rs,
    o_ss,
    o_rs,
):
    S, T = SSPLIT, TSPLIT
    f, tokens = tok_ref.shape
    tl = tokens // T
    R = hbuf.shape[2]
    HB = R * S

    me = lax.axis_index("gx")
    a = me // XS
    b = lax.rem(me, XS)
    p = b // CORES
    core = lax.rem(b, CORES)

    step = 1 - 2 * core
    long_n = G // 2
    short_n = G - 1 - long_n
    group_at = lambda k: lax.rem(a + k * step + G, G)
    long_to = group_at(1) * XS + b
    short_to = group_at(-1) * XS + b
    sibling = a * XS + p * CORES + (1 - core)
    chip = lambda q: a * XS + q * CORES + core
    to = lambda index: {"gx": index}

    loads = [
        pltpu.make_async_copy(gate_hbm.at[0], w_v.at[0], load_sem.at[0]),
        pltpu.make_async_copy(up_hbm.at[0], w_v.at[1], load_sem.at[1]),
        pltpu.make_async_copy(down_hbm.at[0], dt_v, load_sem.at[2]),
    ]
    for c in loads:
        c.start()

    for t in range(T):
        tok[t, a] = tok_ref[:, t * tl : (t + 1) * tl]

    barrier = pltpu.get_barrier_semaphore()
    peers = [long_to, short_to, sibling] + [chip(lax.rem(p + j, Q)) for j in range(1, Q)]
    for peer in peers:
        pl.semaphore_signal(barrier, inc=1, device_id=to(peer), device_id_type=MESH)
    with scope("barrier"):
        pl.semaphore_wait(barrier, len(peers))

    def remote(src, dst, ss, rs, peer):
        return pltpu.make_async_remote_copy(
            src_ref=src, dst_ref=dst, send_sem=ss, recv_sem=rs, device_id=to(peer), device_id_type=MESH
        )

    def ring(buf, ss, rs, i, k, far):
        if far:
            c, peer, e = group_at(-(k - 1)), long_to, k - 1
        else:
            c, peer, e = group_at(k - 1), short_to, long_n + k - 1
        return remote(buf.at[i, c], buf.at[i, c], ss.at[i, e], rs.at[i, e], peer)

    def ring_step(buf, ss, rs, i, k):
        ring(buf, ss, rs, i, k, True).wait_recv()
        if k < long_n:
            ring(buf, ss, rs, i, k + 1, True).start()
        if k <= short_n:
            ring(buf, ss, rs, i, k, False).wait_recv()
            if k < short_n:
                ring(buf, ss, rs, i, k + 1, False).start()

    def ring_start(buf, ss, rs, i):
        ring(buf, ss, rs, i, 1, True).start()
        if short_n:
            ring(buf, ss, rs, i, 1, False).start()

    def ring_drain(buf, ss, rs, i):
        for k in range(1, long_n + 1):
            ring(buf, ss, rs, i, k, True).wait_send()
        for k in range(1, short_n + 1):
            ring(buf, ss, rs, i, k, False).wait_send()

    for t in range(T):
        ring_start(tok, tok_ss, tok_rs, t)

    def turn(load, src, dst):
        load.wait()
        wide = 128

        def body(j, carry):
            j0 = pl.multiple_of(j * wide, wide)
            dst[pl.ds(j0, wide), :] = src[:, pl.ds(j0, wide)].T
            return carry

        lax.fori_loop(0, src.shape[1] // wide, body, 0)

    turns = [(loads[0], w_v.at[0], wt.at[0]), (loads[1], w_v.at[1], wt.at[1]), (loads[2], dt_v, d_v)]
    for k in range(1, long_n + 1):
        if k <= len(turns):
            turn(*turns[k - 1])
        for t in range(T):
            with scope(f"tok#k={k}#t={t}"):
                ring_step(tok, tok_ss, tok_rs, t, k)

    for t in range(T):
        for c in range(G):
            x32[c * f : (c + 1) * f, t * tl : (t + 1) * tl] = tok[t, c].astype(jnp.float32)
    xb[...] = x32[...].astype(jnp.bfloat16)

    def part(q, g, of_core):
        row = pl.multiple_of((q * CORES + of_core) * HB, 32)
        return jnp.dot(wt[g, pl.ds(row, HB), :], xb[...], preferred_element_type=jnp.float32)

    def sib_part(i, carry):
        q, g = i // 2, lax.rem(i, 2)
        r = part(q, g, 1 - core).astype(jnp.bfloat16)
        for s in range(S):
            sib_send[s, q, g] = r[s * R : (s + 1) * R]
        return carry

    with scope("sibpart"):
        lax.fori_loop(0, Q * 2, sib_part, 0)
    sib = [remote(sib_send.at[s], sib_recv.at[s], sib_ss.at[s], sib_rs.at[s], sibling) for s in range(S)]
    for s in range(S):
        sib[s].start()

    def own_part(i, carry):
        q, g = i // 2, lax.rem(i, 2)
        r = part(q, g, core)
        for s in range(S):
            own[s, q, g] = r[s * R : (s + 1) * R]
        return carry

    with scope("ownpart"):
        lax.fori_loop(0, Q * 2, own_part, 0)

    def chain(d, s, q):
        peer = chip(p + 1) if d == 0 else chip(p - 1)
        return remote(ch_send.at[d, s, q], ch_recv.at[d, s, q], ch_ss.at[d, s, q], ch_rs.at[d, s, q], peer)

    def chain_from(d, s, q):
        peer = chip(p - 1) if d == 0 else chip(p + 1)
        return remote(ch_send.at[d, s, q], ch_recv.at[d, s, q], ch_ss.at[d, s, q], ch_rs.at[d, s, q], peer)

    def is_first(d):
        return p == 0 if d == 0 else p == Q - 1

    def sends(d, q):
        return p < q if d == 0 else p > q

    def chain_step(s, depth):
        for d in range(2):

            @pl.when(p == (depth if d == 0 else Q - 1 - depth))
            def _():
                for q in range(Q - 1, depth, -1) if d == 0 else range(Q - 1 - depth):
                    v = own[s, q] + sib_recv[s, q].astype(jnp.float32)
                    if depth > 0:
                        chain_from(d, s, q).wait_recv()
                        v = v + ch_recv[d, s, q].astype(jnp.float32)
                    ch_send[d, s, q] = v.astype(jnp.bfloat16)
                    chain(d, s, q).start()

    def finish(s):
        own[s, p] = own[s, p] + sib_recv[s, p].astype(jnp.float32)
        for d in range(2):

            @pl.when(jnp.logical_not(is_first(d)))
            def _():
                chain_from(d, s, p).wait_recv()
                own[s, p] = own[s, p] + ch_recv[d, s, p].astype(jnp.float32)

        hbuf[s, a] = (gelu(own[s, p, 0]) * own[s, p, 1]).astype(jnp.bfloat16)
        ring_start(hbuf, h_ss, h_rs, s)
        down(s, a)

    def chain_drain(s):
        for d in range(2):
            for q in range(Q):

                @pl.when(sends(d, q))
                def _():
                    chain(d, s, q).wait_send()

    acc[...] = jnp.zeros_like(acc)

    def down(s, c):
        row = pl.multiple_of(c * HB + s * R, 16)
        acc[...] += lax.dot_general(
            d_v[pl.ds(row, R), :], hbuf[s, c], (((0,), (0,)), ((), ())), preferred_element_type=jnp.float32
        )

    def h_step(s, k):
        with scope(f"hwait#s={s}#k={k}"):
            ring_step(hbuf, h_ss, h_rs, s, k)
        down(s, group_at(-k))
        if k <= short_n:
            down(s, group_at(k))

    inner = jnp.logical_and(p > 0, p < Q - 1)
    events = []
    for s in range(S):
        for depth in range(Q - 1):
            events.append((s + depth if depth else 0, 0, s, "chain", depth))
        events.append((s + Q - 2 + 0.1, 1, s, "inner", 0))
        events.append((s + Q - 1, 1, s, "outer", 0))
        for k in range(1, long_n + 1):
            events.append((s + HOLD + k * PACE + 0.2, 2, s, "ring", k))
    for _, _, s, kind, k in sorted(events):
        if kind == "chain":
            if k == 0:
                sib[s].wait_recv()
            with scope(f"chain#s={s}#k={k}"):
                chain_step(s, k)
        elif kind == "ring":
            h_step(s, k)
        else:
            with scope(f"{kind}#s={s}"):

                @pl.when(inner if kind == "inner" else jnp.logical_not(inner))
                def _():
                    finish(s)

    def block(bb):
        return acc[pl.ds(pl.multiple_of(bb * f, 8), f), :]

    for q in range(Q):
        o_sib_send[q] = block(q * CORES + 1 - core).astype(jnp.bfloat16)
    osib = remote(o_sib_send, o_sib_recv, os_ss, os_rs, sibling)
    osib.start()
    with scope("osib"):
        osib.wait_recv()
    outs = []
    for j in range(1, Q):
        q = lax.rem(p + j, Q)
        o_send[j - 1] = (block(q * CORES + core) + o_sib_recv[q].astype(jnp.float32)).astype(jnp.bfloat16)
        c = remote(o_send.at[j - 1], o_recv.at[j - 1], o_ss.at[j - 1], o_rs.at[j - 1], chip(q))
        c.start()
        outs.append(c)
    total = block(b) + o_sib_recv[p].astype(jnp.float32)
    for j, c in enumerate(outs):
        with scope("oout"):
            c.wait_recv()
        total = total + o_recv[j].astype(jnp.float32)
    out_ref[...] = total.astype(jnp.bfloat16)

    for t in range(T):
        ring_drain(tok, tok_ss, tok_rs, t)
    for s in range(S):
        sib[s].wait_send()
        chain_drain(s)
        ring_drain(hbuf, h_ss, h_rs, s)
    osib.wait_send()
    for c in outs:
        c.wait_send()


def shards(G, tokens, gate_weight, up_weight, down_weight):
    f, rows = tokens.shape
    _, depth, width = gate_weight.shape
    _, out_width, down_depth = down_weight.shape
    hb = width // XS
    R = hb // SSPLIT
    bf, f32 = jnp.bfloat16, jnp.float32
    dma = pltpu.SemaphoreType.DMA
    V = pltpu.VMEM
    return pl.pallas_call(
        functools.partial(kernel, G),
        out_shape=jax.ShapeDtypeStruct((f, rows), bf),
        in_specs=[pl.BlockSpec(memory_space=pltpu.VMEM)] + [pl.BlockSpec(memory_space=pl.ANY)] * 3,
        out_specs=pl.BlockSpec(memory_space=pltpu.VMEM),
        scratch_shapes=[
            V((2, depth, width), bf),
            V((out_width, down_depth), bf),
            V((down_depth, out_width), bf),
            V((2, width, depth), bf),
            V((TSPLIT, G, f, rows // TSPLIT), bf),
            V((depth, rows), f32),
            V((depth, rows), bf),
            V((SSPLIT, Q, 2, R, rows), bf),
            V((SSPLIT, Q, 2, R, rows), bf),
            V((SSPLIT, Q, 2, R, rows), f32),
            V((2, SSPLIT, Q, 2, R, rows), bf),
            V((2, SSPLIT, Q, 2, R, rows), bf),
            V((SSPLIT, G, R, rows), bf),
            V((out_width, rows), f32),
            V((Q, f, rows), bf),
            V((Q, f, rows), bf),
            V((Q - 1, f, rows), bf),
            V((Q - 1, f, rows), bf),
            dma((3,)),
            dma((TSPLIT, G - 1)),
            dma((TSPLIT, G - 1)),
            dma((SSPLIT,)),
            dma((SSPLIT,)),
            dma((2, SSPLIT, Q)),
            dma((2, SSPLIT, Q)),
            dma((SSPLIT, G - 1)),
            dma((SSPLIT, G - 1)),
            dma(()),
            dma(()),
            dma((Q - 1,)),
            dma((Q - 1,)),
        ],
        compiler_params=pltpu.CompilerParams(
            collective_id=0, has_side_effects=True, vmem_limit_bytes=60 * 1024 * 1024
        ),
    )(tokens, gate_weight, up_weight, down_weight)


def solution(mesh):
    G = mesh.shape["gx"] // XS
    body = jax.shard_map(
        functools.partial(shards, G),
        mesh=mesh,
        in_specs=(P("gx", "groups"), P("gx", None, None), P("gx", None, None), P("gx", None, None)),
        out_specs=P("gx", "groups"),
        check_vma=False,
    )

    def step(tokens, gate_weight, up_weight, down_weight):
        return body(tokens.T, gate_weight, up_weight, jnp.swapaxes(down_weight, 1, 2)).T

    return step
```

```python
import contextlib
import functools

import jax
import jax.numpy as jnp
from jax import lax
from jax.experimental import pallas as pl
from jax.experimental.pallas import tpu as pltpu
from jax.sharding import PartitionSpec as P

XS = 8
CORES = 2
Q = XS // CORES
LANES = 128
MESH = pl.DeviceIdType.MESH


def scope(name):
    return contextlib.nullcontext()


def gelu(v):
    return 0.5 * v * (1.0 + jnp.tanh(0.7978845608 * (v + 0.044715 * v * v * v)))


def kernel(
    G,
    tok_ref,
    gate_hbm,
    up_hbm,
    down_hbm,
    out_ref,
    w_v,
    dt_v,
    d_v,
    wt,
    tok,
    x32,
    xb,
    sib_send,
    sib_recv,
    own,
    ch_send,
    ch_recv,
    hbuf,
    acc,
    o_sib_send,
    o_sib_recv,
    o_send,
    o_recv,
    load_sem,
    tok_ss,
    tok_rs,
    sib_ss,
    sib_rs,
    ch_ss,
    ch_rs,
    h_ss,
    h_rs,
    os_ss,
    os_rs,
    o_ss,
    o_rs,
):
    f = tok_ref.shape[0]
    T, HB, tl = hbuf.shape[0], hbuf.shape[2], hbuf.shape[3]

    me = lax.axis_index("gx")
    a = me // XS
    b = lax.rem(me, XS)
    p = b // CORES
    core = lax.rem(b, CORES)

    step = 1 - 2 * core
    long_n = G // 2
    short_n = G - 1 - long_n
    group_at = lambda k: lax.rem(a + k * step + G, G)
    long_to = group_at(1) * XS + b
    short_to = group_at(-1) * XS + b
    sibling = a * XS + p * CORES + (1 - core)
    chip = lambda q: a * XS + q * CORES + core
    to = lambda index: {"gx": index}

    loads = [
        pltpu.make_async_copy(gate_hbm.at[0], w_v.at[0], load_sem.at[0]),
        pltpu.make_async_copy(up_hbm.at[0], w_v.at[1], load_sem.at[1]),
        pltpu.make_async_copy(down_hbm.at[0], dt_v, load_sem.at[2]),
    ]
    for t in range(T):
        tok[t, a] = tok_ref[:, t * tl : (t + 1) * tl]

    barrier = pltpu.get_barrier_semaphore()
    peers = [long_to, short_to, sibling] + [chip(lax.rem(p + j, Q)) for j in range(1, Q)]
    for peer in peers:
        pl.semaphore_signal(barrier, inc=1, device_id=to(peer), device_id_type=MESH)
    for c in loads:
        c.start()
    with scope("barrier"):
        pl.semaphore_wait(barrier, len(peers))

    def remote(src, dst, ss, rs, peer):
        return pltpu.make_async_remote_copy(
            src_ref=src, dst_ref=dst, send_sem=ss, recv_sem=rs, device_id=to(peer), device_id_type=MESH
        )

    def ring(buf, ss, rs, i, k, far):
        if far:
            c, peer, e = group_at(-(k - 1)), long_to, k - 1
        else:
            c, peer, e = group_at(k - 1), short_to, long_n + k - 1
        return remote(buf.at[i, c], buf.at[i, c], ss.at[i, e], rs.at[i, e], peer)

    def ring_step(buf, ss, rs, i, k):
        ring(buf, ss, rs, i, k, True).wait_recv()
        if k < long_n:
            ring(buf, ss, rs, i, k + 1, True).start()
        if k <= short_n:
            ring(buf, ss, rs, i, k, False).wait_recv()
            if k < short_n:
                ring(buf, ss, rs, i, k + 1, False).start()

    def ring_start(buf, ss, rs, i):
        ring(buf, ss, rs, i, 1, True).start()
        if short_n:
            ring(buf, ss, rs, i, 1, False).start()

    def ring_drain(buf, ss, rs, i):
        for k in range(1, long_n + 1):
            ring(buf, ss, rs, i, k, True).wait_send()
        for k in range(1, short_n + 1):
            ring(buf, ss, rs, i, k, False).wait_send()

    def turn(load, src, dst):
        load.wait()
        wide = 128

        def body(j, carry):
            j0 = pl.multiple_of(j * wide, wide)
            dst[pl.ds(j0, wide), :] = src[:, pl.ds(j0, wide)].T
            return carry

        lax.fori_loop(0, src.shape[1] // wide, body, 0)

    turns = [(loads[0], w_v.at[0], wt.at[0]), (loads[1], w_v.at[1], wt.at[1]), (loads[2], dt_v, d_v)]

    def sums(t):
        for c in range(G):
            x32[c * f : (c + 1) * f, :] = tok[t, c].astype(jnp.float32)
        xb[...] = x32[...].astype(jnp.bfloat16)

        def part(q, g, of_core):
            row = pl.multiple_of((q * CORES + of_core) * HB, 32)
            return jnp.dot(wt[g, pl.ds(row, HB), :], xb[...], preferred_element_type=jnp.float32)

        def sib_part(i, carry):
            q, g = i // 2, lax.rem(i, 2)
            sib_send[t, q, g] = part(q, g, 1 - core).astype(jnp.bfloat16)
            return carry

        def own_part(i, carry):
            q, g = i // 2, lax.rem(i, 2)
            own[t, q, g] = part(q, g, core)
            return carry

        lax.fori_loop(0, Q * 2, sib_part, 0)
        pair(t).start()
        lax.fori_loop(0, Q * 2, own_part, 0)

    def pair(t):
        return remote(sib_send.at[t], sib_recv.at[t], sib_ss.at[t], sib_rs.at[t], sibling)

    def chain(d, s, q):
        peer = chip(p + 1) if d == 0 else chip(p - 1)
        return remote(ch_send.at[d, s, q], ch_recv.at[d, s, q], ch_ss.at[d, s, q], ch_rs.at[d, s, q], peer)

    def chain_from(d, s, q):
        peer = chip(p - 1) if d == 0 else chip(p + 1)
        return remote(ch_send.at[d, s, q], ch_recv.at[d, s, q], ch_ss.at[d, s, q], ch_rs.at[d, s, q], peer)

    def is_first(d):
        return p == 0 if d == 0 else p == Q - 1

    def sends(d, q):
        return p < q if d == 0 else p > q

    def chain_step(s, depth):
        for d in range(2):

            @pl.when(p == (depth if d == 0 else Q - 1 - depth))
            def _():
                for q in range(Q - 1, depth, -1) if d == 0 else range(Q - 1 - depth):
                    v = own[s, q] + sib_recv[s, q].astype(jnp.float32)
                    if depth > 0:
                        chain_from(d, s, q).wait_recv()
                        v = v + ch_recv[d, s, q].astype(jnp.float32)
                    ch_send[d, s, q] = v.astype(jnp.bfloat16)
                    chain(d, s, q).start()

    def finish(s):
        own[s, p] = own[s, p] + sib_recv[s, p].astype(jnp.float32)
        for d in range(2):

            @pl.when(jnp.logical_not(is_first(d)))
            def _():
                chain_from(d, s, p).wait_recv()
                own[s, p] = own[s, p] + ch_recv[d, s, p].astype(jnp.float32)

        hbuf[s, a] = (gelu(own[s, p, 0]) * own[s, p, 1]).astype(jnp.bfloat16)
        ring_start(hbuf, h_ss, h_rs, s)
        down(s, a)

    def chain_drain(s):
        for d in range(2):
            for q in range(Q):

                @pl.when(sends(d, q))
                def _():
                    chain(d, s, q).wait_send()

    acc[...] = jnp.zeros_like(acc)

    def down(s, c):
        row = pl.multiple_of(c * HB, 32)
        acc[s] += lax.dot_general(
            d_v[pl.ds(row, HB), :], hbuf[s, c], (((0,), (0,)), ((), ())), preferred_element_type=jnp.float32
        )

    def h_step(s, k):
        with scope(f"hwait#s={s}#k={k}"):
            ring_step(hbuf, h_ss, h_rs, s, k)
        down(s, group_at(-k))
        if k <= short_n:
            down(s, group_at(k))

    def block(s, bb):
        return acc[s, pl.ds(pl.multiple_of(bb * f, 8), f), :]

    def out_pair(s):
        return remote(o_sib_send.at[s], o_sib_recv.at[s], os_ss.at[s], os_rs.at[s], sibling)

    def out_to(s, j):
        peer = chip(lax.rem(p + j, Q))
        return remote(o_send.at[s, j - 1], o_recv.at[s, j - 1], o_ss.at[s, j - 1], o_rs.at[s, j - 1], peer)

    def out_step(s, stage):
        if stage == 0:
            for q in range(Q):
                o_sib_send[s, q] = block(s, q * CORES + 1 - core).astype(jnp.bfloat16)
            out_pair(s).start()
        elif stage == 1:
            out_pair(s).wait_recv()
            for j in range(1, Q):
                q = lax.rem(p + j, Q)
                v = block(s, q * CORES + core) + o_sib_recv[s, q].astype(jnp.float32)
                o_send[s, j - 1] = v.astype(jnp.bfloat16)
                out_to(s, j).start()
        else:
            total = block(s, b) + o_sib_recv[s, p].astype(jnp.float32)
            for j in range(1, Q):
                out_to(s, j).wait_recv()
                total = total + o_recv[s, j - 1].astype(jnp.float32)
            out_ref[:, s * tl : (s + 1) * tl] = total.astype(jnp.bfloat16)

    inner = jnp.logical_and(p > 0, p < Q - 1)
    events = []
    for s in range(T):
        for k in range(1, long_n + 1):
            events.append((5.5 * k + 1.9 * s, s, "tokens", k))
        start = 24.0 + 3.5 * s
        events.append((start, s, "sums", 0))
        events.append((start + 0.1, s, "chain", 0))
        base = 25.0 + 10.0 * s
        for depth in range(1, Q - 1):
            events.append((base + 3.5 + 5.0 * depth, s, "chain", depth))
        events.append((base + 17.0, s, "inner", 0))
        events.append((base + 19.0, s, "outer", 0))
        for k in range(1, long_n + 1):
            events.append((base + 21.0 + 11.0 * k, s, "ring", k))
        last = base + 21.0 + 11.0 * long_n
        for stage, after in enumerate((0.1, 3.0, 10.0)):
            events.append((last + after, s, "out", stage))

    for t in range(T):
        ring_start(tok, tok_ss, tok_rs, t)
        if t < len(turns):
            with scope(f"turn#t={t}"):
                turn(*turns[t])
    for t in range(T, len(turns)):
        turn(*turns[t])
    for _, s, kind, k in sorted(events):
        if kind == "tokens":
            with scope(f"tok#s={s}#k={k}"):
                ring_step(tok, tok_ss, tok_rs, s, k)
        elif kind == "sums":
            with scope(f"sums#s={s}"):
                sums(s)
        elif kind == "chain":
            if k == 0:
                pair(s).wait_recv()
            with scope(f"chain#s={s}#k={k}"):
                chain_step(s, k)
        elif kind == "ring":
            h_step(s, k)
        elif kind == "out":
            with scope(f"out#s={s}#k={k}"):
                out_step(s, k)
        else:
            with scope(f"{kind}#s={s}"):

                @pl.when(inner if kind == "inner" else jnp.logical_not(inner))
                def _():
                    finish(s)

    for s in range(T):
        ring_drain(tok, tok_ss, tok_rs, s)
        pair(s).wait_send()
        chain_drain(s)
        ring_drain(hbuf, h_ss, h_rs, s)
        out_pair(s).wait_send()
        for j in range(1, Q):
            out_to(s, j).wait_send()


def shards(G, tokens, gate_weight, up_weight, down_weight):
    f, rows = tokens.shape
    _, depth, width = gate_weight.shape
    _, out_width, down_depth = down_weight.shape
    hb = width // XS
    T = rows // LANES
    bf, f32 = jnp.bfloat16, jnp.float32
    dma = pltpu.SemaphoreType.DMA
    V = pltpu.VMEM
    return pl.pallas_call(
        functools.partial(kernel, G),
        out_shape=jax.ShapeDtypeStruct((f, rows), bf),
        in_specs=[pl.BlockSpec(memory_space=pltpu.VMEM)] + [pl.BlockSpec(memory_space=pl.ANY)] * 3,
        out_specs=pl.BlockSpec(memory_space=pltpu.VMEM),
        scratch_shapes=[
            V((2, depth, width), bf),
            V((out_width, down_depth), bf),
            V((down_depth, out_width), bf),
            V((2, width, depth), bf),
            V((T, G, f, LANES), bf),
            V((depth, LANES), f32),
            V((depth, LANES), bf),
            V((T, Q, 2, hb, LANES), bf),
            V((T, Q, 2, hb, LANES), bf),
            V((T, Q, 2, hb, LANES), f32),
            V((2, T, Q, 2, hb, LANES), bf),
            V((2, T, Q, 2, hb, LANES), bf),
            V((T, G, hb, LANES), bf),
            V((T, out_width, LANES), f32),
            V((T, Q, f, LANES), bf),
            V((T, Q, f, LANES), bf),
            V((T, Q - 1, f, LANES), bf),
            V((T, Q - 1, f, LANES), bf),
            dma((3,)),
            dma((T, G - 1)),
            dma((T, G - 1)),
            dma((T,)),
            dma((T,)),
            dma((2, T, Q)),
            dma((2, T, Q)),
            dma((T, G - 1)),
            dma((T, G - 1)),
            dma((T,)),
            dma((T,)),
            dma((T, Q - 1)),
            dma((T, Q - 1)),
        ],
        compiler_params=pltpu.CompilerParams(
            collective_id=0, has_side_effects=True, vmem_limit_bytes=60 * 1024 * 1024
        ),
    )(tokens, gate_weight, up_weight, down_weight)


def solution(mesh):
    G = mesh.shape["gx"] // XS
    body = jax.shard_map(
        functools.partial(shards, G),
        mesh=mesh,
        in_specs=(P("gx", "groups"), P("gx", None, None), P("gx", None, None), P("gx", None, None)),
        out_specs=P("gx", "groups"),
        check_vma=False,
    )

    def step(tokens, gate_weight, up_weight, down_weight):
        return body(tokens.T, gate_weight, up_weight, jnp.swapaxes(down_weight, 1, 2)).T

    return step
```

```python
import contextlib
import functools

import jax
import jax.numpy as jnp
from jax import lax
from jax.experimental import pallas as pl
from jax.experimental.pallas import tpu as pltpu
from jax.sharding import PartitionSpec as P

XS = 8
CORES = 2
Q = XS // CORES
LANES = 128
HALVES = 2
MESH = pl.DeviceIdType.MESH


def scope(name):
    return contextlib.nullcontext()


def gelu(v):
    return 0.5 * v * (1.0 + jnp.tanh(0.7978845608 * (v + 0.044715 * v * v * v)))


def kernel(
    G,
    tok_ref,
    gate_hbm,
    up_hbm,
    down_hbm,
    out_ref,
    w_v,
    dt_v,
    d_v,
    wt,
    tok,
    x32,
    xb,
    sib_send,
    sib_recv,
    own,
    ch_send,
    ch_recv,
    hbuf,
    acc,
    o_sib_send,
    o_sib_recv,
    o_send,
    o_recv,
    load_sem,
    tok_ss,
    tok_rs,
    sib_ss,
    sib_rs,
    ch_ss,
    ch_rs,
    h_ss,
    h_rs,
    os_ss,
    os_rs,
    o_ss,
    o_rs,
):
    f = tok_ref.shape[0]
    T, HB, tl = own.shape[0], own.shape[3], own.shape[4]
    HR = HB // HALVES
    S = T * HALVES
    rows_of = lambda s: slice((s % HALVES) * HR, (s % HALVES + 1) * HR)

    me = lax.axis_index("gx")
    a = me // XS
    b = lax.rem(me, XS)
    p = b // CORES
    core = lax.rem(b, CORES)

    step = 1 - 2 * core
    long_n = G // 2
    short_n = G - 1 - long_n
    group_at = lambda k: lax.rem(a + k * step + G, G)
    long_to = group_at(1) * XS + b
    short_to = group_at(-1) * XS + b
    sibling = a * XS + p * CORES + (1 - core)
    chip = lambda q: a * XS + q * CORES + core
    to = lambda index: {"gx": index}

    loads = [
        pltpu.make_async_copy(gate_hbm.at[0], w_v.at[0], load_sem.at[0]),
        pltpu.make_async_copy(up_hbm.at[0], w_v.at[1], load_sem.at[1]),
        pltpu.make_async_copy(down_hbm.at[0], dt_v, load_sem.at[2]),
    ]
    for t in range(T):
        tok[t, a] = tok_ref[:, t * tl : (t + 1) * tl]

    barrier = pltpu.get_barrier_semaphore()
    peers = [long_to, short_to, sibling] + [chip(lax.rem(p + j, Q)) for j in range(1, Q)]
    for peer in peers:
        pl.semaphore_signal(barrier, inc=1, device_id=to(peer), device_id_type=MESH)
    for c in loads:
        c.start()
    with scope("barrier"):
        pl.semaphore_wait(barrier, len(peers))

    def remote(src, dst, ss, rs, peer):
        return pltpu.make_async_remote_copy(
            src_ref=src, dst_ref=dst, send_sem=ss, recv_sem=rs, device_id=to(peer), device_id_type=MESH
        )

    def ring(buf, ss, rs, i, k, far):
        if far:
            c, peer, e = group_at(-(k - 1)), long_to, k - 1
        else:
            c, peer, e = group_at(k - 1), short_to, long_n + k - 1
        return remote(buf.at[i, c], buf.at[i, c], ss.at[i, e], rs.at[i, e], peer)

    def ring_step(buf, ss, rs, i, k):
        ring(buf, ss, rs, i, k, True).wait_recv()
        if k < long_n:
            ring(buf, ss, rs, i, k + 1, True).start()
        if k <= short_n:
            ring(buf, ss, rs, i, k, False).wait_recv()
            if k < short_n:
                ring(buf, ss, rs, i, k + 1, False).start()

    def ring_start(buf, ss, rs, i):
        ring(buf, ss, rs, i, 1, True).start()
        if short_n:
            ring(buf, ss, rs, i, 1, False).start()

    def ring_drain(buf, ss, rs, i):
        for k in range(1, long_n + 1):
            ring(buf, ss, rs, i, k, True).wait_send()
        for k in range(1, short_n + 1):
            ring(buf, ss, rs, i, k, False).wait_send()

    def turn(load, src, dst):
        load.wait()
        wide = 128

        def body(j, carry):
            j0 = pl.multiple_of(j * wide, wide)
            dst[pl.ds(j0, wide), :] = src[:, pl.ds(j0, wide)].T
            return carry

        lax.fori_loop(0, src.shape[1] // wide, body, 0)

    turns = [(loads[0], w_v.at[0], wt.at[0]), (loads[1], w_v.at[1], wt.at[1]), (loads[2], dt_v, d_v)]

    def sums(t):
        for c in range(G):
            x32[c * f : (c + 1) * f, :] = tok[t, c].astype(jnp.float32)
        xb[...] = x32[...].astype(jnp.bfloat16)

        def part(q, g, of_core):
            row = pl.multiple_of((q * CORES + of_core) * HB, 32)
            return jnp.dot(wt[g, pl.ds(row, HB), :], xb[...], preferred_element_type=jnp.float32)

        def sib_part(j, carry):
            q = first_q(j)
            for g in range(2):
                sib_send[t, q, g] = part(q, g, 1 - core).astype(jnp.bfloat16)
            pair(t, q).start()
            return carry

        lax.fori_loop(0, Q, sib_part, 0)
        for j in range(Q):
            q = first_q(j)
            for g in range(2):
                own[t, q, g] = part(q, g, core)
            pair(t, q).wait_recv()
            if j < Q - 1:
                for s in range(t * HALVES, (t + 1) * HALVES):
                    for d, qs in ((0, Q - 1 - j), (1, j)):

                        @pl.when(is_first(d))
                        def _():
                            ch_send[d, s, qs] = chip_sum(s, qs).astype(jnp.bfloat16)
                            chain(d, s, qs).start()

    def first_q(j):
        low = 1 - p // (Q // 2)
        return low * (Q - 1 - j) + (1 - low) * j

    def pair(t, q):
        return remote(sib_send.at[t, q], sib_recv.at[t, q], sib_ss.at[t, q], sib_rs.at[t, q], sibling)

    def chip_sum(s, q):
        t = s // HALVES
        return own[t, q, :, rows_of(s)] + sib_recv[t, q, :, rows_of(s)].astype(jnp.float32)

    def chain(d, s, q):
        peer = chip(p + 1) if d == 0 else chip(p - 1)
        return remote(ch_send.at[d, s, q], ch_recv.at[d, s, q], ch_ss.at[d, s, q], ch_rs.at[d, s, q], peer)

    def chain_from(d, s, q):
        peer = chip(p - 1) if d == 0 else chip(p + 1)
        return remote(ch_send.at[d, s, q], ch_recv.at[d, s, q], ch_ss.at[d, s, q], ch_rs.at[d, s, q], peer)

    def is_first(d):
        return p == 0 if d == 0 else p == Q - 1

    def sends(d, q):
        return p < q if d == 0 else p > q

    def chain_step(s, depth):
        for d in range(2):

            @pl.when(p == (depth if d == 0 else Q - 1 - depth))
            def _():
                for q in range(Q - 1, depth, -1) if d == 0 else range(Q - 1 - depth):
                    v = chip_sum(s, q)
                    chain_from(d, s, q).wait_recv()
                    v = v + ch_recv[d, s, q].astype(jnp.float32)
                    ch_send[d, s, q] = v.astype(jnp.bfloat16)
                    chain(d, s, q).start()

    def finish(s):
        t = s // HALVES
        own[t, p, :, rows_of(s)] = chip_sum(s, p)
        for d in range(2):

            @pl.when(jnp.logical_not(is_first(d)))
            def _():
                chain_from(d, s, p).wait_recv()
                own[t, p, :, rows_of(s)] = own[t, p, :, rows_of(s)] + ch_recv[d, s, p].astype(jnp.float32)

        hbuf[s, a] = (gelu(own[t, p, 0, rows_of(s)]) * own[t, p, 1, rows_of(s)]).astype(jnp.bfloat16)
        ring_start(hbuf, h_ss, h_rs, s)
        down(s, a)

    def chain_drain(s):
        for d in range(2):
            for q in range(Q):

                @pl.when(sends(d, q))
                def _():
                    chain(d, s, q).wait_send()

    acc[...] = jnp.zeros_like(acc)

    def down(s, c):
        row = pl.multiple_of(c * HB + (s % HALVES) * HR, 16)
        acc[s // HALVES] += lax.dot_general(
            d_v[pl.ds(row, HR), :], hbuf[s, c], (((0,), (0,)), ((), ())), preferred_element_type=jnp.float32
        )

    def h_step(s, k):
        with scope(f"hwait#s={s}#k={k}"):
            ring_step(hbuf, h_ss, h_rs, s, k)
        down(s, group_at(-k))
        if k <= short_n:
            down(s, group_at(k))

    def block(s, bb):
        return acc[s, pl.ds(pl.multiple_of(bb * f, 8), f), :]

    def out_pair(s):
        return remote(o_sib_send.at[s], o_sib_recv.at[s], os_ss.at[s], os_rs.at[s], sibling)

    def out_to(s, j):
        peer = chip(lax.rem(p + j, Q))
        return remote(o_send.at[s, j - 1], o_recv.at[s, j - 1], o_ss.at[s, j - 1], o_rs.at[s, j - 1], peer)

    def out_step(s, stage):
        if stage == 0:
            for q in range(Q):
                o_sib_send[s, q] = block(s, q * CORES + 1 - core).astype(jnp.bfloat16)
            out_pair(s).start()
        elif stage == 1:
            out_pair(s).wait_recv()
            for j in range(1, Q):
                q = lax.rem(p + j, Q)
                v = block(s, q * CORES + core) + o_sib_recv[s, q].astype(jnp.float32)
                o_send[s, j - 1] = v.astype(jnp.bfloat16)
                out_to(s, j).start()
        else:
            total = block(s, b) + o_sib_recv[s, p].astype(jnp.float32)
            for j in range(1, Q):
                out_to(s, j).wait_recv()
                total = total + o_recv[s, j - 1].astype(jnp.float32)
            out_ref[:, s * tl : (s + 1) * tl] = total.astype(jnp.bfloat16)

    inner = jnp.logical_and(p > 0, p < Q - 1)
    events = []
    for t in range(T):
        for k in range(1, long_n + 1):
            events.append((5.7 * k + 1.9 * t, t, "tokens", k))
        events.append((23.0 + 4.5 * t, t, "sums", 0))
    for s in range(S):
        base = 26.0 + 4.8 * s
        for depth in range(1, Q - 1):
            events.append((base + 2.5 + 3.5 * depth, s, "chain", depth))
        events.append((base + 11.0, s, "inner", 0))
        events.append((base + 13.5, s, "outer", 0))
        for k in range(1, long_n + 1):
            last = base + 9.0 + 13.5 * k
            events.append((last, s, "ring", k))
        if (s + 1) % HALVES == 0:
            for stage, after in enumerate((0.1, 2.0, 10.0)):
                events.append((last + after, s // HALVES, "out", stage))

    for t in range(T):
        ring_start(tok, tok_ss, tok_rs, t)
        if t < len(turns):
            with scope(f"turn#t={t}"):
                turn(*turns[t])
    for t in range(T, len(turns)):
        turn(*turns[t])
    for _, s, kind, k in sorted(events):
        if kind == "tokens":
            with scope(f"tok#s={s}#k={k}"):
                ring_step(tok, tok_ss, tok_rs, s, k)
        elif kind == "sums":
            with scope(f"sums#s={s}"):
                sums(s)
        elif kind == "chain":
            with scope(f"chain#s={s}#k={k}"):
                chain_step(s, k)
        elif kind == "ring":
            h_step(s, k)
        elif kind == "out":
            with scope(f"out#s={s}#k={k}"):
                out_step(s, k)
        else:
            with scope(f"{kind}#s={s}"):

                @pl.when(inner if kind == "inner" else jnp.logical_not(inner))
                def _():
                    finish(s)

    for t in range(T):
        ring_drain(tok, tok_ss, tok_rs, t)
        for q in range(Q):
            pair(t, q).wait_send()
        out_pair(t).wait_send()
        for j in range(1, Q):
            out_to(t, j).wait_send()
    for s in range(S):
        chain_drain(s)
        ring_drain(hbuf, h_ss, h_rs, s)


def shards(G, tokens, gate_weight, up_weight, down_weight):
    f, rows = tokens.shape
    _, depth, width = gate_weight.shape
    _, out_width, down_depth = down_weight.shape
    hb = width // XS
    T = rows // LANES
    S, hr = T * HALVES, hb // HALVES
    bf, f32 = jnp.bfloat16, jnp.float32
    dma = pltpu.SemaphoreType.DMA
    V = pltpu.VMEM
    return pl.pallas_call(
        functools.partial(kernel, G),
        out_shape=jax.ShapeDtypeStruct((f, rows), bf),
        in_specs=[pl.BlockSpec(memory_space=pltpu.VMEM)] + [pl.BlockSpec(memory_space=pl.ANY)] * 3,
        out_specs=pl.BlockSpec(memory_space=pltpu.VMEM),
        scratch_shapes=[
            V((2, depth, width), bf),
            V((out_width, down_depth), bf),
            V((down_depth, out_width), bf),
            V((2, width, depth), bf),
            V((T, G, f, LANES), bf),
            V((depth, LANES), f32),
            V((depth, LANES), bf),
            V((T, Q, 2, hb, LANES), bf),
            V((T, Q, 2, hb, LANES), bf),
            V((T, Q, 2, hb, LANES), f32),
            V((2, S, Q, 2, hr, LANES), bf),
            V((2, S, Q, 2, hr, LANES), bf),
            V((S, G, hr, LANES), bf),
            V((T, out_width, LANES), f32),
            V((T, Q, f, LANES), bf),
            V((T, Q, f, LANES), bf),
            V((T, Q - 1, f, LANES), bf),
            V((T, Q - 1, f, LANES), bf),
            dma((3,)),
            dma((T, G - 1)),
            dma((T, G - 1)),
            dma((T, Q)),
            dma((T, Q)),
            dma((2, S, Q)),
            dma((2, S, Q)),
            dma((S, G - 1)),
            dma((S, G - 1)),
            dma((T,)),
            dma((T,)),
            dma((T, Q - 1)),
            dma((T, Q - 1)),
        ],
        compiler_params=pltpu.CompilerParams(
            collective_id=0, has_side_effects=True, vmem_limit_bytes=60 * 1024 * 1024
        ),
    )(tokens, gate_weight, up_weight, down_weight)


def solution(mesh):
    G = mesh.shape["gx"] // XS
    body = jax.shard_map(
        functools.partial(shards, G),
        mesh=mesh,
        in_specs=(P("gx", "groups"), P("gx", None, None), P("gx", None, None), P("gx", None, None)),
        out_specs=P("gx", "groups"),
        check_vma=False,
    )

    def step(tokens, gate_weight, up_weight, down_weight):
        return body(tokens.T, gate_weight, up_weight, jnp.swapaxes(down_weight, 1, 2)).T

    return step
```

```python
import contextlib
import functools

import jax
import jax.numpy as jnp
from jax import lax
from jax.experimental import pallas as pl
from jax.experimental.pallas import tpu as pltpu
from jax.sharding import PartitionSpec as P

XS = 8
CORES = 2
Q = XS // CORES
LANES = 128
HALVES = 2
MESH = pl.DeviceIdType.MESH


def scope(name):
    return contextlib.nullcontext()


def gelu(v):
    return 0.5 * v * (1.0 + jnp.tanh(0.7978845608 * (v + 0.044715 * v * v * v)))


def kernel(
    G,
    tok_ref,
    gate_hbm,
    up_hbm,
    down_hbm,
    out_ref,
    w_v,
    dt_v,
    d_v,
    wt,
    tok,
    x32,
    xb,
    sib_send,
    sib_recv,
    own,
    ch_send,
    ch_recv,
    hbuf,
    h_in,
    acc,
    o_sib_send,
    o_sib_recv,
    o_send,
    o_recv,
    load_sem,
    tok_ss,
    tok_rs,
    sib_ss,
    sib_rs,
    ch_ss,
    ch_rs,
    h_ss,
    h_rs,
    in_ss,
    in_rs,
    os_ss,
    os_rs,
    o_ss,
    o_rs,
):
    f = tok_ref.shape[0]
    T, HB, tl = own.shape[0], own.shape[3], own.shape[4]
    HR = HB // HALVES
    S = T * HALVES
    rows_of = lambda s: slice((s % HALVES) * HR, (s % HALVES + 1) * HR)

    me = lax.axis_index("gx")
    a = me // XS
    b = lax.rem(me, XS)
    p = b // CORES
    core = lax.rem(b, CORES)

    step = 1 - 2 * core
    long_n = G // 2
    short_n = G - 1 - long_n
    group_at = lambda k: lax.rem(a + k * step + G, G)
    long_to = group_at(1) * XS + b
    short_to = group_at(-1) * XS + b
    sibling = a * XS + p * CORES + (1 - core)
    chip = lambda q: a * XS + q * CORES + core
    to = lambda index: {"gx": index}

    upper = p // (Q // 2)
    inner_p = 1 + upper * (Q - 3)
    outer_p = upper * (Q - 1)
    is_inner = jnp.logical_and(p > 0, p < Q - 1)
    beyond = lax.rem(a + 2 * upper - 1 + G, G)
    before = lax.rem(a - 2 * upper + 1 + G, G)
    beyond_far = upper * (1 - core) + (1 - upper) * core
    end_peer = beyond * XS + inner_p * CORES + core
    inner_peer = before * XS + outer_p * CORES + core
    inside = lax.rem((p + 1) // 2, 2)
    cross = inside * inner_peer + (1 - inside) * end_peer

    loads = [
        pltpu.make_async_copy(gate_hbm.at[0], w_v.at[0], load_sem.at[0]),
        pltpu.make_async_copy(up_hbm.at[0], w_v.at[1], load_sem.at[1]),
        pltpu.make_async_copy(down_hbm.at[0], dt_v, load_sem.at[2]),
    ]
    for t in range(T):
        tok[t, a] = tok_ref[:, t * tl : (t + 1) * tl]

    barrier = pltpu.get_barrier_semaphore()
    peers = [long_to, short_to, sibling, cross] + [chip(lax.rem(p + j, Q)) for j in range(1, Q)]
    for peer in peers:
        pl.semaphore_signal(barrier, inc=1, device_id=to(peer), device_id_type=MESH)
    for c in loads:
        c.start()
    with scope("barrier"):
        pl.semaphore_wait(barrier, len(peers))

    def remote(src, dst, ss, rs, peer):
        return pltpu.make_async_remote_copy(
            src_ref=src, dst_ref=dst, send_sem=ss, recv_sem=rs, device_id=to(peer), device_id_type=MESH
        )

    def ring(buf, ss, rs, i, k, far):
        if far:
            c, peer, e = group_at(-(k - 1)), long_to, k - 1
        else:
            c, peer, e = group_at(k - 1), short_to, long_n + k - 1
        return remote(buf.at[i, c], buf.at[i, c], ss.at[i, e], rs.at[i, e], peer)

    def ring_step(buf, ss, rs, i, k):
        ring(buf, ss, rs, i, k, True).wait_recv()
        if k < long_n:
            ring(buf, ss, rs, i, k + 1, True).start()
        if k <= short_n:
            ring(buf, ss, rs, i, k, False).wait_recv()
            if k < short_n:
                ring(buf, ss, rs, i, k + 1, False).start()

    def ring_start(buf, ss, rs, i):
        ring(buf, ss, rs, i, 1, True).start()
        if short_n:
            ring(buf, ss, rs, i, 1, False).start()

    def ring_drain(buf, ss, rs, i):
        for k in range(1, long_n + 1):
            ring(buf, ss, rs, i, k, True).wait_send()
        for k in range(1, short_n + 1):
            ring(buf, ss, rs, i, k, False).wait_send()

    def turn(load, src, dst):
        load.wait()
        wide = 128

        def body(j, carry):
            j0 = pl.multiple_of(j * wide, wide)
            dst[pl.ds(j0, wide), :] = src[:, pl.ds(j0, wide)].T
            return carry

        lax.fori_loop(0, src.shape[1] // wide, body, 0)

    turns = [(loads[0], w_v.at[0], wt.at[0]), (loads[1], w_v.at[1], wt.at[1]), (loads[2], dt_v, d_v)]

    def sums(t):
        for c in range(G):
            x32[c * f : (c + 1) * f, :] = tok[t, c].astype(jnp.float32)
        xb[...] = x32[...].astype(jnp.bfloat16)

        def part(q, g, of_core):
            row = pl.multiple_of((q * CORES + of_core) * HB, 32)
            return jnp.dot(wt[g, pl.ds(row, HB), :], xb[...], preferred_element_type=jnp.float32)

        def sib_part(j, carry):
            q = first_q(j)
            for g in range(2):
                sib_send[t, q, g] = part(q, g, 1 - core).astype(jnp.bfloat16)
            pair(t, q).start()
            return carry

        lax.fori_loop(0, Q, sib_part, 0)
        for j in range(Q):
            q = first_q(j)
            for g in range(2):
                own[t, q, g] = part(q, g, core)
            pair(t, q).wait_recv()
            if j < Q // 2:
                for s in range(t * HALVES, (t + 1) * HALVES):
                    for d in range(2):

                        @pl.when(p == d * (Q - 1))
                        def _():
                            chain_send(s, of_direction(d)[j], False)

    def first_q(j):
        h = j // (Q // 2)
        low = (1 - h) * (Q // 2 + j) + h * (Q - 1 - j)
        return (1 - upper) * low + upper * (Q - 1 - low)

    def pair(t, q):
        return remote(sib_send.at[t, q], sib_recv.at[t, q], sib_ss.at[t, q], sib_rs.at[t, q], sibling)

    def chip_sum(s, q):
        t = s // HALVES
        return own[t, q, :, rows_of(s)] + sib_recv[t, q, :, rows_of(s)].astype(jnp.float32)

    def of_direction(d):
        return list(range(Q // 2, Q)) if d == 0 else list(reversed(range(Q // 2)))

    def chain(s, q, peer):
        return remote(ch_send.at[s, q], ch_recv.at[s, q], ch_ss.at[s, q], ch_rs.at[s, q], peer)

    def chain_to(s, q):
        return chain(s, q, chip(p + 1) if q >= Q // 2 else chip(p - 1))

    def chain_send(s, q, adds):
        v = chip_sum(s, q)
        if adds:
            chain_to(s, q).wait_recv()
            v = v + ch_recv[s, q].astype(jnp.float32)
        ch_send[s, q] = v.astype(jnp.bfloat16)
        chain_to(s, q).start()

    def chain_step(s, depth):
        for d in range(2):

            @pl.when(p == (depth if d == 0 else Q - 1 - depth))
            def _():
                for q in of_direction(d):
                    chain_send(s, q, True)

    def to_inner(s):
        return remote(h_in.at[s], hbuf.at[s, a], in_ss.at[s, 0], in_rs.at[s], chip(inner_p))

    def to_beyond(s):
        e = (1 - beyond_far) * long_n
        return remote(h_in.at[s], hbuf.at[s, a], in_ss.at[s, 1], h_rs.at[s, e], end_peer)

    def finish(s):
        t = s // HALVES

        def hidden(q):
            own[t, q, :, rows_of(s)] = chip_sum(s, q)
            chain(s, q, chip(inner_p)).wait_recv()
            own[t, q, :, rows_of(s)] = own[t, q, :, rows_of(s)] + ch_recv[s, q].astype(jnp.float32)
            return (gelu(own[t, q, 0, rows_of(s)]) * own[t, q, 1, rows_of(s)]).astype(jnp.bfloat16)

        h_in[s] = hidden(inner_p)
        to_inner(s).start()
        to_beyond(s).start()
        hbuf[s, a] = hidden(p)
        ring_start(hbuf, h_ss, h_rs, s)
        down(s, a)

    def take(s):
        to_inner(s).wait_recv()
        inward(s, lambda copy: copy.start())
        down(s, a)

    def inward(s, act):
        @pl.when(beyond_far == 0)
        def _():
            act(ring(hbuf, h_ss, h_rs, s, 1, True))

        @pl.when(beyond_far == 1)
        def _():
            act(ring(hbuf, h_ss, h_rs, s, 1, False))

    def chain_drain(s):
        for q in range(Q):

            @pl.when(p < Q - 1 if q >= Q // 2 else p > 0)
            def _():
                chain_to(s, q).wait_send()

    def hidden_drain(s):
        for k in range(2, long_n + 1):
            ring(hbuf, h_ss, h_rs, s, k, True).wait_send()
        for k in range(2, short_n + 1):
            ring(hbuf, h_ss, h_rs, s, k, False).wait_send()

        @pl.when(is_inner)
        def _():
            inward(s, lambda copy: copy.wait_send())

        @pl.when(jnp.logical_not(is_inner))
        def _():
            ring(hbuf, h_ss, h_rs, s, 1, True).wait_send()
            ring(hbuf, h_ss, h_rs, s, 1, False).wait_send()
            to_inner(s).wait_send()
            to_beyond(s).wait_send()

    acc[...] = jnp.zeros_like(acc)

    def down(s, c):
        row = pl.multiple_of(c * HB + (s % HALVES) * HR, 16)
        acc[s // HALVES] += lax.dot_general(
            d_v[pl.ds(row, HR), :], hbuf[s, c], (((0,), (0,)), ((), ())), preferred_element_type=jnp.float32
        )

    def h_step(s, k):
        with scope(f"hwait#s={s}#k={k}"):
            ring_step(hbuf, h_ss, h_rs, s, k)
        down(s, group_at(-k))
        if k <= short_n:
            down(s, group_at(k))

    def block(s, bb):
        return acc[s, pl.ds(pl.multiple_of(bb * f, 8), f), :]

    def out_pair(s):
        return remote(o_sib_send.at[s], o_sib_recv.at[s], os_ss.at[s], os_rs.at[s], sibling)

    def out_to(s, j):
        peer = chip(lax.rem(p + j, Q))
        return remote(o_send.at[s, j - 1], o_recv.at[s, j - 1], o_ss.at[s, j - 1], o_rs.at[s, j - 1], peer)

    def out_step(s, stage):
        if stage == 0:
            for q in range(Q):
                o_sib_send[s, q] = block(s, q * CORES + 1 - core).astype(jnp.bfloat16)
            out_pair(s).start()
        elif stage == 1:
            out_pair(s).wait_recv()
            for j in range(1, Q):
                q = lax.rem(p + j, Q)
                v = block(s, q * CORES + core) + o_sib_recv[s, q].astype(jnp.float32)
                o_send[s, j - 1] = v.astype(jnp.bfloat16)
                out_to(s, j).start()
        else:
            total = block(s, b) + o_sib_recv[s, p].astype(jnp.float32)
            for j in range(1, Q):
                out_to(s, j).wait_recv()
                total = total + o_recv[s, j - 1].astype(jnp.float32)
            out_ref[:, s * tl : (s + 1) * tl] = total.astype(jnp.bfloat16)

    events = []
    for t in range(T):
        for k in range(1, long_n + 1):
            events.append((5.7 * k + 1.9 * t, t, "tokens", k))
        events.append((23.0 + 3.2 * t, t, "sums", 0))
    for s in range(S):
        base = 26.0 + 4.0 * s
        for depth in range(1, Q - 1):
            events.append((base + 1.0 + 4.0 * depth, s, "chain", depth))
        events.append((base + 13.0, s, "finish", 0))
        events.append((base + 15.9, s, "take", 0))
        for k in range(1, long_n + 1):
            last = 53.0 + 5.5 * s + 13.5 * (k - 1)
            events.append((last, s, "ring", k))
        if s < S - 1:
            events.append((last + 3.0, s, "drain", 0))
        if (s + 1) % HALVES == 0:
            for stage, after in enumerate((0.1, 2.0, 10.0)):
                events.append((last + after, s // HALVES, "out", stage))

    for t in range(T):
        ring_start(tok, tok_ss, tok_rs, t)
        if t < len(turns):
            with scope(f"turn#t={t}"):
                turn(*turns[t])
    for t in range(T, len(turns)):
        turn(*turns[t])
    for _, s, kind, k in sorted(events):
        if kind == "tokens":
            with scope(f"tok#s={s}#k={k}"):
                ring_step(tok, tok_ss, tok_rs, s, k)
        elif kind == "sums":
            with scope(f"sums#s={s}"):
                sums(s)
        elif kind == "chain":
            with scope(f"chain#s={s}#k={k}"):
                chain_step(s, k)
        elif kind == "ring":
            h_step(s, k)
        elif kind == "out":
            with scope(f"out#s={s}#k={k}"):
                out_step(s, k)
        elif kind == "drain":
            chain_drain(s)
            hidden_drain(s)
            if s < T:
                ring_drain(tok, tok_ss, tok_rs, s)
                for q in range(Q):
                    pair(s, q).wait_send()
        elif kind == "finish":
            with scope(f"finish#s={s}"):
                pl.when(jnp.logical_not(is_inner))(functools.partial(finish, s))
        else:
            with scope(f"take#s={s}"):
                pl.when(is_inner)(functools.partial(take, s))

    chain_drain(S - 1)
    hidden_drain(S - 1)
    for t in range(T):
        out_pair(t).wait_send()
        for j in range(1, Q):
            out_to(t, j).wait_send()


def shards(G, tokens, gate_weight, up_weight, down_weight):
    f, rows = tokens.shape
    _, depth, width = gate_weight.shape
    _, out_width, down_depth = down_weight.shape
    hb = width // XS
    T = rows // LANES
    S, hr = T * HALVES, hb // HALVES
    bf, f32 = jnp.bfloat16, jnp.float32
    dma = pltpu.SemaphoreType.DMA
    V = pltpu.VMEM
    return pl.pallas_call(
        functools.partial(kernel, G),
        out_shape=jax.ShapeDtypeStruct((f, rows), bf),
        in_specs=[pl.BlockSpec(memory_space=pltpu.VMEM)] + [pl.BlockSpec(memory_space=pl.ANY)] * 3,
        out_specs=pl.BlockSpec(memory_space=pltpu.VMEM),
        scratch_shapes=[
            V((2, depth, width), bf),
            V((out_width, down_depth), bf),
            V((down_depth, out_width), bf),
            V((2, width, depth), bf),
            V((T, G, f, LANES), bf),
            V((depth, LANES), f32),
            V((depth, LANES), bf),
            V((T, Q, 2, hb, LANES), bf),
            V((T, Q, 2, hb, LANES), bf),
            V((T, Q, 2, hb, LANES), f32),
            V((S, Q, 2, hr, LANES), bf),
            V((S, Q, 2, hr, LANES), bf),
            V((S, G, hr, LANES), bf),
            V((S, hr, LANES), bf),
            V((T, out_width, LANES), f32),
            V((T, Q, f, LANES), bf),
            V((T, Q, f, LANES), bf),
            V((T, Q - 1, f, LANES), bf),
            V((T, Q - 1, f, LANES), bf),
            dma((3,)),
            dma((T, G - 1)),
            dma((T, G - 1)),
            dma((T, Q)),
            dma((T, Q)),
            dma((S, Q)),
            dma((S, Q)),
            dma((S, G - 1)),
            dma((S, G - 1)),
            dma((S, 2)),
            dma((S,)),
            dma((T,)),
            dma((T,)),
            dma((T, Q - 1)),
            dma((T, Q - 1)),
        ],
        compiler_params=pltpu.CompilerParams(
            collective_id=0, has_side_effects=True, vmem_limit_bytes=60 * 1024 * 1024
        ),
    )(tokens, gate_weight, up_weight, down_weight)


def solution(mesh):
    G = mesh.shape["gx"] // XS
    body = jax.shard_map(
        functools.partial(shards, G),
        mesh=mesh,
        in_specs=(P("gx", "groups"), P("gx", None, None), P("gx", None, None), P("gx", None, None)),
        out_specs=P("gx", "groups"),
        check_vma=False,
    )

    def step(tokens, gate_weight, up_weight, down_weight):
        return body(tokens.T, gate_weight, up_weight, jnp.swapaxes(down_weight, 1, 2)).T

    return step
```

```python
import contextlib
import functools

import jax
import jax.numpy as jnp
from jax import lax
from jax.experimental import pallas as pl
from jax.experimental.pallas import tpu as pltpu
from jax.sharding import PartitionSpec as P

XS = 8
CORES = 2
Q = XS // CORES
LANES = 128
HALVES = 2
MESH = pl.DeviceIdType.MESH


def scope(name):
    return contextlib.nullcontext()


def gelu(v):
    return 0.5 * v * (1.0 + jnp.tanh(0.7978845608 * (v + 0.044715 * v * v * v)))


def kernel(
    G,
    tok_ref,
    gate_hbm,
    up_hbm,
    down_hbm,
    out_ref,
    w_v,
    dt_v,
    d_v,
    wt,
    tok,
    x32,
    xb,
    sib_send,
    sib_recv,
    own,
    ch_send,
    ch_recv,
    hbuf,
    acc,
    o_sib_send,
    o_sib_recv,
    o_send,
    o_recv,
    load_sem,
    tok_ss,
    tok_rs,
    sib_ss,
    sib_rs,
    ch_ss,
    ch_rs,
    h_ss,
    h_rs,
    os_ss,
    os_rs,
    o_ss,
    o_rs,
):
    f = tok_ref.shape[0]
    T, HB, tl = own.shape[0], own.shape[3], own.shape[4]
    HR = HB // HALVES
    S = T * HALVES
    rows_of = lambda s: slice((s % HALVES) * HR, (s % HALVES + 1) * HR)

    me = lax.axis_index("gx")
    a = me // XS
    b = lax.rem(me, XS)
    p = b // CORES
    core = lax.rem(b, CORES)

    step = 1 - 2 * core
    long_n = G // 2
    short_n = G - 1 - long_n
    group_at = lambda k: lax.rem(a + k * step + G, G)
    long_to = group_at(1) * XS + b
    short_to = group_at(-1) * XS + b
    sibling = a * XS + p * CORES + (1 - core)
    chip = lambda q: a * XS + q * CORES + core
    to = lambda index: {"gx": index}

    loads = [
        pltpu.make_async_copy(gate_hbm.at[0], w_v.at[0], load_sem.at[0]),
        pltpu.make_async_copy(up_hbm.at[0], w_v.at[1], load_sem.at[1]),
        pltpu.make_async_copy(down_hbm.at[0], dt_v, load_sem.at[2]),
    ]
    for t in range(T):
        tok[t, a] = tok_ref[:, t * tl : (t + 1) * tl]

    barrier = pltpu.get_barrier_semaphore()
    peers = [long_to, short_to, sibling] + [chip(lax.rem(p + j, Q)) for j in range(1, Q)]
    for peer in peers:
        pl.semaphore_signal(barrier, inc=1, device_id=to(peer), device_id_type=MESH)
    for c in loads:
        c.start()
    with scope("barrier"):
        pl.semaphore_wait(barrier, len(peers))

    def remote(src, dst, ss, rs, peer):
        return pltpu.make_async_remote_copy(
            src_ref=src, dst_ref=dst, send_sem=ss, recv_sem=rs, device_id=to(peer), device_id_type=MESH
        )

    def ring(buf, ss, rs, i, k, far):
        if far:
            c, peer, e = group_at(-(k - 1)), long_to, k - 1
        else:
            c, peer, e = group_at(k - 1), short_to, long_n + k - 1
        return remote(buf.at[i, c], buf.at[i, c], ss.at[i, e], rs.at[i, e], peer)

    def ring_step(buf, ss, rs, i, k):
        ring(buf, ss, rs, i, k, True).wait_recv()
        if k < long_n:
            ring(buf, ss, rs, i, k + 1, True).start()
        if k <= short_n:
            ring(buf, ss, rs, i, k, False).wait_recv()
            if k < short_n:
                ring(buf, ss, rs, i, k + 1, False).start()

    def ring_start(buf, ss, rs, i):
        ring(buf, ss, rs, i, 1, True).start()
        if short_n:
            ring(buf, ss, rs, i, 1, False).start()

    def ring_drain(buf, ss, rs, i):
        for k in range(1, long_n + 1):
            ring(buf, ss, rs, i, k, True).wait_send()
        for k in range(1, short_n + 1):
            ring(buf, ss, rs, i, k, False).wait_send()

    def turn(load, src, dst):
        load.wait()
        wide = 128

        def body(j, carry):
            j0 = pl.multiple_of(j * wide, wide)
            dst[pl.ds(j0, wide), :] = src[:, pl.ds(j0, wide)].T
            return carry

        lax.fori_loop(0, src.shape[1] // wide, body, 0)

    turns = [(loads[0], w_v.at[0], wt.at[0]), (loads[1], w_v.at[1], wt.at[1]), (loads[2], dt_v, d_v)]

    def sums(t):
        for c in range(G):
            x32[c * f : (c + 1) * f, :] = tok[t, c].astype(jnp.float32)
        xb[...] = x32[...].astype(jnp.bfloat16)

        def part(q, g, of_core):
            row = pl.multiple_of((q * CORES + of_core) * HB, 32)
            return jnp.dot(wt[g, pl.ds(row, HB), :], xb[...], preferred_element_type=jnp.float32)

        def sib_part(j, carry):
            q = first_q(j)
            for g in range(2):
                sib_send[t, q, g] = part(q, g, 1 - core).astype(jnp.bfloat16)
            pair(t, q).start()
            return carry

        lax.fori_loop(0, Q, sib_part, 0)
        for j in range(Q):
            q = first_q(j)
            for g in range(2):
                own[t, q, g] = part(q, g, core)
            pair(t, q).wait_recv()
            if j < Q - 1:
                for s in range(t * HALVES, (t + 1) * HALVES):
                    for d, qs in ((0, Q - 1 - j), (1, j)):

                        @pl.when(is_first(d))
                        def _():
                            ch_send[d, s, qs] = chip_sum(s, qs).astype(jnp.bfloat16)
                            chain(d, s, qs).start()

    def first_q(j):
        low = 1 - p // (Q // 2)
        return low * (Q - 1 - j) + (1 - low) * j

    def pair(t, q):
        return remote(sib_send.at[t, q], sib_recv.at[t, q], sib_ss.at[t, q], sib_rs.at[t, q], sibling)

    def chip_sum(s, q):
        t = s // HALVES
        return own[t, q, :, rows_of(s)] + sib_recv[t, q, :, rows_of(s)].astype(jnp.float32)

    def chain(d, s, q):
        peer = chip(p + 1) if d == 0 else chip(p - 1)
        return remote(ch_send.at[d, s, q], ch_recv.at[d, s, q], ch_ss.at[d, s, q], ch_rs.at[d, s, q], peer)

    def chain_from(d, s, q):
        peer = chip(p - 1) if d == 0 else chip(p + 1)
        return remote(ch_send.at[d, s, q], ch_recv.at[d, s, q], ch_ss.at[d, s, q], ch_rs.at[d, s, q], peer)

    def is_first(d):
        return p == 0 if d == 0 else p == Q - 1

    def sends(d, q):
        return p < q if d == 0 else p > q

    def chain_step(s, depth):
        for d in range(2):

            @pl.when(p == (depth if d == 0 else Q - 1 - depth))
            def _():
                for q in range(Q - 1, depth, -1) if d == 0 else range(Q - 1 - depth):
                    v = chip_sum(s, q)
                    chain_from(d, s, q).wait_recv()
                    v = v + ch_recv[d, s, q].astype(jnp.float32)
                    ch_send[d, s, q] = v.astype(jnp.bfloat16)
                    chain(d, s, q).start()

    def finish(s):
        t = s // HALVES
        own[t, p, :, rows_of(s)] = chip_sum(s, p)
        for d in range(2):

            @pl.when(jnp.logical_not(is_first(d)))
            def _():
                chain_from(d, s, p).wait_recv()
                own[t, p, :, rows_of(s)] = own[t, p, :, rows_of(s)] + ch_recv[d, s, p].astype(jnp.float32)

        hbuf[s, a] = (gelu(own[t, p, 0, rows_of(s)]) * own[t, p, 1, rows_of(s)]).astype(jnp.bfloat16)
        ring_start(hbuf, h_ss, h_rs, s)
        down(s, a)

    def chain_drain(s):
        for d in range(2):
            for q in range(Q):

                @pl.when(sends(d, q))
                def _():
                    chain(d, s, q).wait_send()

    acc[...] = jnp.zeros_like(acc)

    def down(s, c):
        row = pl.multiple_of(c * HB + (s % HALVES) * HR, 16)
        acc[s // HALVES] += lax.dot_general(
            d_v[pl.ds(row, HR), :], hbuf[s, c], (((0,), (0,)), ((), ())), preferred_element_type=jnp.float32
        )

    def h_step(s, k):
        with scope(f"hwait#s={s}#k={k}"):
            ring_step(hbuf, h_ss, h_rs, s, k)
        down(s, group_at(-k))
        if k <= short_n:
            down(s, group_at(k))

    def block(s, bb):
        return acc[s, pl.ds(pl.multiple_of(bb * f, 8), f), :]

    def out_pair(s):
        return remote(o_sib_send.at[s], o_sib_recv.at[s], os_ss.at[s], os_rs.at[s], sibling)

    def out_to(s, j):
        peer = chip(lax.rem(p + j, Q))
        return remote(o_send.at[s, j - 1], o_recv.at[s, j - 1], o_ss.at[s, j - 1], o_rs.at[s, j - 1], peer)

    def out_step(s, stage):
        if stage == 0:
            for q in range(Q):
                o_sib_send[s, q] = block(s, q * CORES + 1 - core).astype(jnp.bfloat16)
            out_pair(s).start()
        elif stage == 1:
            out_pair(s).wait_recv()
            for j in range(1, Q):
                q = lax.rem(p + j, Q)
                v = block(s, q * CORES + core) + o_sib_recv[s, q].astype(jnp.float32)
                o_send[s, j - 1] = v.astype(jnp.bfloat16)
                out_to(s, j).start()
        else:
            total = block(s, b) + o_sib_recv[s, p].astype(jnp.float32)
            for j in range(1, Q):
                out_to(s, j).wait_recv()
                total = total + o_recv[s, j - 1].astype(jnp.float32)
            out_ref[:, s * tl : (s + 1) * tl] = total.astype(jnp.bfloat16)

    inner = jnp.logical_and(p > 0, p < Q - 1)
    events = []
    for t in range(T):
        for k in range(1, long_n + 1):
            events.append((5.7 * k + 1.9 * t, t, "tokens", k))
        events.append((23.0 + 4.5 * t, t, "sums", 0))
    for s in range(S):
        base = 26.0 + 4.8 * s
        for depth in range(1, Q - 1):
            events.append((base + 2.5 + 3.5 * depth, s, "chain", depth))
        events.append((base + 11.0, s, "inner", 0))
        events.append((base + 13.5, s, "outer", 0))
        for k in range(1, long_n + 1):
            last = base + 9.0 + 13.5 * k
            events.append((last, s, "ring", k))
        if s < S - 1:
            events.append((last + 3.0, s, "drain", 0))
        if (s + 1) % HALVES == 0:
            for stage, after in enumerate((0.1, 2.0, 10.0)):
                events.append((last + after, s // HALVES, "out", stage))

    for t in range(T):
        ring_start(tok, tok_ss, tok_rs, t)
        if t < len(turns):
            with scope(f"turn#t={t}"):
                turn(*turns[t])
    for t in range(T, len(turns)):
        turn(*turns[t])
    for _, s, kind, k in sorted(events):
        if kind == "tokens":
            with scope(f"tok#s={s}#k={k}"):
                ring_step(tok, tok_ss, tok_rs, s, k)
        elif kind == "sums":
            with scope(f"sums#s={s}"):
                sums(s)
        elif kind == "chain":
            with scope(f"chain#s={s}#k={k}"):
                chain_step(s, k)
        elif kind == "ring":
            h_step(s, k)
        elif kind == "drain":
            chain_drain(s)
            ring_drain(hbuf, h_ss, h_rs, s)
            if s < T:
                ring_drain(tok, tok_ss, tok_rs, s)
                for q in range(Q):
                    pair(s, q).wait_send()
        elif kind == "out":
            with scope(f"out#s={s}#k={k}"):
                out_step(s, k)
        else:
            with scope(f"{kind}#s={s}"):

                @pl.when(inner if kind == "inner" else jnp.logical_not(inner))
                def _():
                    finish(s)

    chain_drain(S - 1)
    ring_drain(hbuf, h_ss, h_rs, S - 1)
    for t in range(T):
        out_pair(t).wait_send()
        for j in range(1, Q):
            out_to(t, j).wait_send()


def shards(G, tokens, gate_weight, up_weight, down_weight):
    f, rows = tokens.shape
    _, depth, width = gate_weight.shape
    _, out_width, down_depth = down_weight.shape
    hb = width // XS
    T = rows // LANES
    S, hr = T * HALVES, hb // HALVES
    bf, f32 = jnp.bfloat16, jnp.float32
    dma = pltpu.SemaphoreType.DMA
    V = pltpu.VMEM
    return pl.pallas_call(
        functools.partial(kernel, G),
        out_shape=jax.ShapeDtypeStruct((f, rows), bf),
        in_specs=[pl.BlockSpec(memory_space=pltpu.VMEM)] + [pl.BlockSpec(memory_space=pl.ANY)] * 3,
        out_specs=pl.BlockSpec(memory_space=pltpu.VMEM),
        scratch_shapes=[
            V((2, depth, width), bf),
            V((out_width, down_depth), bf),
            V((down_depth, out_width), bf),
            V((2, width, depth), bf),
            V((T, G, f, LANES), bf),
            V((depth, LANES), f32),
            V((depth, LANES), bf),
            V((T, Q, 2, hb, LANES), bf),
            V((T, Q, 2, hb, LANES), bf),
            V((T, Q, 2, hb, LANES), f32),
            V((2, S, Q, 2, hr, LANES), bf),
            V((2, S, Q, 2, hr, LANES), bf),
            V((S, G, hr, LANES), bf),
            V((T, out_width, LANES), f32),
            V((T, Q, f, LANES), bf),
            V((T, Q, f, LANES), bf),
            V((T, Q - 1, f, LANES), bf),
            V((T, Q - 1, f, LANES), bf),
            dma((3,)),
            dma((T, G - 1)),
            dma((T, G - 1)),
            dma((T, Q)),
            dma((T, Q)),
            dma((2, S, Q)),
            dma((2, S, Q)),
            dma((S, G - 1)),
            dma((S, G - 1)),
            dma((T,)),
            dma((T,)),
            dma((T, Q - 1)),
            dma((T, Q - 1)),
        ],
        compiler_params=pltpu.CompilerParams(
            collective_id=0, has_side_effects=True, vmem_limit_bytes=60 * 1024 * 1024
        ),
    )(tokens, gate_weight, up_weight, down_weight)


def solution(mesh):
    G = mesh.shape["gx"] // XS
    body = jax.shard_map(
        functools.partial(shards, G),
        mesh=mesh,
        in_specs=(P("gx", "groups"), P("gx", None, None), P("gx", None, None), P("gx", None, None)),
        out_specs=P("gx", "groups"),
        check_vma=False,
    )

    def step(tokens, gate_weight, up_weight, down_weight):
        return body(tokens.T, gate_weight, up_weight, jnp.swapaxes(down_weight, 1, 2)).T

    return step
```
